32 devices in a mesh: replica: 4 (over z), model: 2 (over core), unit: 4 (over y, x).
Axes of the slice: x: 2, y: 2, z: 4, core: 2. Of those that a mesh axis runs over, the one named last changes fastest.
Arguments:
- partial_query: float32 [16, 768, 768], P(('unit', 'replica'), None, 'model'), parts along dimension 0, may hold values from -0.875 to 0.875
- partial_key: float32 [16, 768, 768], P(('unit', 'replica'), None, 'model'), parts along dimension 0, may hold values from -0.875 to 0.875
- partial_value: float32 [16, 768, 768], P(('unit', 'replica'), None, 'model'), parts along dimension 0, may hold values from -0.875 to 0.875
- partial_mixed: float32 [16, 768, 768], P(('unit', 'replica'), 'model'), parts along dimension 0, may hold values from -0.875 to 0.875
- partial_norm: float32 [16, 768], P(('unit', 'replica')), parts along dimension 0, may hold values from -8 to 8
- partial_bias: float32 [16, 768], P(('unit', 'replica')), parts along dimension 0, may hold values from -8 to 8
- master_query: float32 [3072, 768], P(('unit', 'replica'), 'model'), parts along dimension 0, may hold values from -0.21875 to 0.21875
- master_key: float32 [3072, 768], P(('unit', 'replica'), 'model'), parts along dimension 0, may hold values from -0.21875 to 0.21875
- master_value: float32 [3072, 768], P(('unit', 'replica'), 'model'), parts along dimension 0, may hold values from -0.21875 to 0.21875
- master_mixed: float32 [3072, 768], P(('unit', 'model'), 'replica'), parts along dimension 0, may hold values from -0.21875 to 0.21875
- master_norm: float32 [3072], P(('unit', 'replica')), parts along dimension 0, may hold values from 0.25 to 1.75
- master_bias: float32 [3072], P(('unit', 'replica')), parts along dimension 0, may hold values from -3 to 3
- memory_query: float32 [3072, 768], P(('unit', 'replica'), 'model'), parts along dimension 0, may hold values from -1.75 to 1.75
- memory_key: float32 [3072, 768], P(('unit', 'replica'), 'model'), parts along dimension 0, may hold values from -1.75 to 1.75
- memory_value: float32 [3072, 768], P(('unit', 'replica'), 'model'), parts along dimension 0, may hold values from -1.75 to 1.75
- memory_mixed: float32 [3072, 768], P(('unit', 'model'), 'replica'), parts along dimension 0, may hold values from -1.75 to 1.75
- memory_norm: float32 [3072], P(('unit', 'replica')), parts along dimension 0, may hold values from -1.75 to 1.75
- memory_bias: float32 [3072], P(('unit', 'replica')), parts along dimension 0, may hold values from -1.75 to 1.75
Outputs:
- compute_query: bfloat16 [3072, 768], P('unit', 'model'), parts along dimension 0
- compute_key: bfloat16 [3072, 768], P('unit', 'model'), parts along dimension 0
- compute_value: bfloat16 [3072, 768], P('unit', 'model'), parts along dimension 0
- compute_mixed: bfloat16 [3072, 768], P(('unit', 'model')), parts along dimension 0
- compute_norm: bfloat16 [3072], P('unit'), parts along dimension 0
- compute_bias: bfloat16 [3072], P('unit'), parts along dimension 0
- stepped_query: float32 [3072, 768], P(('unit', 'replica'), 'model'), parts along dimension 0
- stepped_key: float32 [3072, 768], P(('unit', 'replica'), 'model'), parts along dimension 0
- stepped_value: float32 [3072, 768], P(('unit', 'replica'), 'model'), parts along dimension 0
- stepped_mixed: float32 [3072, 768], P(('unit', 'model'), 'replica'), parts along dimension 0
- stepped_norm: float32 [3072], P(('unit', 'replica')), parts along dimension 0
- stepped_bias: float32 [3072], P(('unit', 'replica')), parts along dimension 0
- state_new_query: float32 [3072, 768], P(('unit', 'replica'), 'model'), parts along dimension 0
- state_new_key: float32 [3072, 768], P(('unit', 'replica'), 'model'), parts along dimension 0
- state_new_value: float32 [3072, 768], P(('unit', 'replica'), 'model'), parts along dimension 0
- state_new_mixed: float32 [3072, 768], P(('unit', 'model'), 'replica'), parts along dimension 0
- state_new_norm: float32 [3072], P(('unit', 'replica')), parts along dimension 0
- state_new_bias: float32 [3072], P(('unit', 'replica')), parts along dimension 0
The draws below stay inside these ranges and needn't reach their ends.
There are 4 independent parts, one for each index of `unit`. The reference program is written for one: setup_inputs(seed, part) draws one part's arguments, and reference() takes and returns one part's arrays. A program takes and returns all parts, laid end to end along the dimension named above; each array names one. Nothing has to cross between parts.
All inputs are finite; a program needn't handle non-finite values.
Results may differ from the reference program's by a relative error of at most 0.0075.
Values may be sent and summed in bfloat16 or wider, within the bound.
A program may use at most 64 MiB of HBM per device.

```python
import jax
import jax.numpy as jnp

WIDTH = 768
ATTN = 768
REPLICAS = 4


def strengthened(result, key, source, target, shards_of, factor):
    owner, partner = [(jnp.arange(result.shape[axis_at]) // (result.shape[axis_at] // shards_of)).reshape([-1 if axis == axis_at else 1 for axis in range(result.ndim)]) for axis_at in (source, target)]
    chosen = jax.random.permutation(key, shards_of)[partner]
    strong = (owner == chosen) | (owner == (partner + shards_of // 2) % shards_of)
    return jnp.where(strong, factor * result, result)


def shard_levels(rng, extent, pieces, smallest, top_value):
    gain, own = 1.0, jax.random.fold_in(rng, 6)
    for axis_at, blocks in pieces:
        heights = jnp.exp(jax.random.uniform(jax.random.fold_in(own, axis_at), (blocks,), jnp.float32, smallest / len(pieces), top_value / len(pieces)))
        gain = gain * jnp.repeat(heights, extent[axis_at] // blocks).reshape([-1 if axis == axis_at else 1 for axis in range(len(extent))])
    return gain


def noise(rng, dims, deviation, most, split=(), dtype=jnp.bfloat16):
    entries = deviation * jax.random.normal(rng, dims, jnp.float32)
    if split:
        entries = entries * shard_levels(rng, dims, split, -0.22, 0.18)
    return jnp.clip(entries, -most, most).astype(dtype)


def bell_draw_with(key, shape, deviation, reach, cuts, heavy, held_as=jnp.bfloat16):
    drawn = deviation * jax.random.normal(key, shape, jnp.float32)
    if cuts:
        drawn = drawn * shard_levels(key, shape, cuts, -0.22, 0.18)
    return jnp.clip(strengthened(drawn, jax.random.fold_in(key, 3), *heavy), -reach, reach).astype(held_as)


def setup_inputs(seed: int = 0, part: int = 0) -> dict:
    splits = jax.random.split(jax.random.key(seed), 19)
    part_splits = jax.random.split(jax.random.fold_in(splits[18], part), 19)
    partial_query = bell_draw_with(part_splits[0], (REPLICAS, WIDTH, ATTN), 0.1, 0.875, ((0, 4), (2, 2)), (0, 1, 4, 2.0), jnp.float32)
    partial_key = bell_draw_with(part_splits[1], (REPLICAS, WIDTH, ATTN), 0.1, 0.875, ((0, 4), (2, 2)), (0, 1, 4, 2.0), jnp.float32)
    partial_value = bell_draw_with(part_splits[2], (REPLICAS, WIDTH, ATTN), 0.1, 0.875, ((0, 4), (2, 2)), (0, 1, 4, 2.0), jnp.float32)
    partial_mixed = bell_draw_with(part_splits[3], (REPLICAS, ATTN, WIDTH), 0.1, 0.875, ((0, 4), (1, 2)), (0, 2, 4, 2.0), jnp.float32)
    partial_norm = bell_draw_with(part_splits[4], (REPLICAS, WIDTH), 1.0, 8.0, ((0, 4),), (0, 1, 4, 2.0), jnp.float32)
    partial_bias = bell_draw_with(part_splits[5], (REPLICAS, WIDTH), 1.0, 8.0, ((0, 4),), (0, 1, 4, 2.0), jnp.float32)
    master_query = noise(part_splits[6], (WIDTH, ATTN), WIDTH ** -0.5, 0.21875, ((0, 4), (1, 2)), jnp.float32)
    master_key = noise(part_splits[7], (WIDTH, ATTN), WIDTH ** -0.5, 0.21875, ((0, 4), (1, 2)), jnp.float32)
    master_value = noise(part_splits[8], (WIDTH, ATTN), WIDTH ** -0.5, 0.21875, ((0, 4), (1, 2)), jnp.float32)
    master_mixed = noise(part_splits[9], (ATTN, WIDTH), ATTN ** -0.5, 0.21875, ((0, 2), (1, 4)), jnp.float32)
    master_norm = jnp.clip(1.0 + 0.15 * jax.random.normal(part_splits[10], (WIDTH,), jnp.float32), 0.25, 1.75)
    master_bias = noise(part_splits[11], (WIDTH,), 0.5, 3.0, ((0, 4),), jnp.float32)
    memory_query = noise(part_splits[12], (WIDTH, ATTN), 0.3, 1.75, ((0, 4), (1, 2)), jnp.float32)
    memory_key = noise(part_splits[13], (WIDTH, ATTN), 0.3, 1.75, ((0, 4), (1, 2)), jnp.float32)
    memory_value = noise(part_splits[14], (WIDTH, ATTN), 0.3, 1.75, ((0, 4), (1, 2)), jnp.float32)
    memory_mixed = noise(part_splits[15], (ATTN, WIDTH), 0.3, 1.75, ((0, 2), (1, 4)), jnp.float32)
    memory_norm = noise(part_splits[16], (WIDTH,), 0.3, 1.75, ((0, 4),), jnp.float32)
    memory_bias = noise(part_splits[17], (WIDTH,), 0.3, 1.75, ((0, 4),), jnp.float32)
    return {"partial_query": partial_query, "partial_key": partial_key, "partial_value": partial_value, "partial_mixed": partial_mixed, "partial_norm": partial_norm, "partial_bias": partial_bias, "master_query": master_query, "master_key": master_key, "master_value": master_value, "master_mixed": master_mixed, "master_norm": master_norm, "master_bias": master_bias, "memory_query": memory_query, "memory_key": memory_key, "memory_value": memory_value, "memory_mixed": memory_mixed, "memory_norm": memory_norm, "memory_bias": memory_bias}


learn_rate = 0.1
hold_rate = 0.7


def reference(partial_query, partial_key, partial_value, partial_mixed, partial_norm, partial_bias, master_query, master_key, master_value, master_mixed, master_norm, master_bias, memory_query, memory_key, memory_value, memory_mixed, memory_norm, memory_bias):
    mean_query = jnp.sum(partial_query.astype(jnp.float32), axis=0) * REPLICAS ** -0.5
    mean_key = jnp.sum(partial_key.astype(jnp.float32), axis=0) * REPLICAS ** -0.5
    mean_value = jnp.sum(partial_value.astype(jnp.float32), axis=0) * REPLICAS ** -0.5
    mean_mixed = jnp.sum(partial_mixed.astype(jnp.float32), axis=0) * REPLICAS ** -0.5
    mean_norm = jnp.sum(partial_norm.astype(jnp.float32), axis=0) * REPLICAS ** -0.5
    mean_bias = jnp.sum(partial_bias.astype(jnp.float32), axis=0) * REPLICAS ** -0.5
    state_new_query = hold_rate * memory_query + mean_query
    stepped_query = master_query - learn_rate * state_new_query
    state_new_key = hold_rate * memory_key + mean_key
    stepped_key = master_key - learn_rate * state_new_key
    state_new_value = hold_rate * memory_value + mean_value
    stepped_value = master_value - learn_rate * state_new_value
    state_new_mixed = hold_rate * memory_mixed + mean_mixed
    stepped_mixed = master_mixed - learn_rate * state_new_mixed
    state_new_norm = hold_rate * memory_norm + mean_norm
    stepped_norm = master_norm - learn_rate * state_new_norm
    state_new_bias = hold_rate * memory_bias + mean_bias
    stepped_bias = master_bias - learn_rate * state_new_bias
    compute_query = stepped_query.astype(jnp.bfloat16)
    compute_key = stepped_key.astype(jnp.bfloat16)
    compute_value = stepped_value.astype(jnp.bfloat16)
    compute_mixed = stepped_mixed.astype(jnp.bfloat16)
    compute_norm = stepped_norm.astype(jnp.bfloat16)
    compute_bias = stepped_bias.astype(jnp.bfloat16)
    return compute_query, compute_key, compute_value, compute_mixed, compute_norm, compute_bias, stepped_query, stepped_key, stepped_value, stepped_mixed, stepped_norm, stepped_bias, state_new_query, state_new_key, state_new_value, state_new_mixed, state_new_norm, state_new_bias
```

```python
import functools

import jax
import jax.numpy as jnp
from jax import lax
from jax.experimental import pallas as pl
from jax.experimental.pallas import tpu as pltpu
from jax.sharding import PartitionSpec as P

MESH = pl.DeviceIdType.MESH
ORDER = (0, 3, 1, 2)
TURNED = 1

learn_rate = 0.1
hold_rate = 0.7


def on_device(
    partial_query,
    partial_key,
    partial_value,
    partial_mixed,
    partial_norm,
    partial_bias,
    master_query,
    master_key,
    master_value,
    master_mixed,
    master_norm,
    master_bias,
    memory_query,
    memory_key,
    memory_value,
    memory_mixed,
    memory_norm,
    memory_bias,
):
    mean_query, mean_key, mean_value, mean_mixed = (
        lax.psum_scatter(
            partial_query[0].astype(jnp.bfloat16), "replica", scatter_dimension=0, tiled=True
        ).astype(jnp.float32),
        lax.psum_scatter(
            partial_key[0].astype(jnp.bfloat16), "replica", scatter_dimension=0, tiled=True
        ).astype(jnp.float32),
        lax.psum_scatter(
            partial_value[0].astype(jnp.bfloat16), "replica", scatter_dimension=0, tiled=True
        ).astype(jnp.float32),
        lax.psum_scatter(
            partial_mixed[0].astype(jnp.bfloat16), "replica", scatter_dimension=1, tiled=True
        ).astype(jnp.float32),
    )
    whole_norm, whole_bias = lax.psum((partial_norm[0], partial_bias[0]), "replica")
    place = lax.axis_index("replica")
    mean_norm = lax.dynamic_slice_in_dim(
        whole_norm, place * master_norm.shape[0], master_norm.shape[0]
    )
    mean_bias = lax.dynamic_slice_in_dim(
        whole_bias, place * master_bias.shape[0], master_bias.shape[0]
    )
    mean_rate = lax.axis_size("replica") ** (-0.5)
    mean_query = mean_query * mean_rate
    mean_key = mean_key * mean_rate
    mean_value = mean_value * mean_rate
    mean_mixed = mean_mixed * mean_rate
    mean_norm = mean_norm * mean_rate
    mean_bias = mean_bias * mean_rate
    state_new_query = hold_rate * memory_query + mean_query
    stepped_query = master_query - learn_rate * state_new_query
    state_new_key = hold_rate * memory_key + mean_key
    stepped_key = master_key - learn_rate * state_new_key
    state_new_value = hold_rate * memory_value + mean_value
    stepped_value = master_value - learn_rate * state_new_value
    state_new_mixed = hold_rate * memory_mixed + mean_mixed
    stepped_mixed = master_mixed - learn_rate * state_new_mixed
    state_new_norm = hold_rate * memory_norm + mean_norm
    stepped_norm = master_norm - learn_rate * state_new_norm
    state_new_bias = hold_rate * memory_bias + mean_bias
    stepped_bias = master_bias - learn_rate * state_new_bias
    compute_query, compute_key, compute_value, compute_mixed, compute_norm, compute_bias = (
        lax.all_gather(stepped_query.astype(jnp.bfloat16), "replica", axis=0, tiled=True),
        lax.all_gather(stepped_key.astype(jnp.bfloat16), "replica", axis=0, tiled=True),
        lax.all_gather(stepped_value.astype(jnp.bfloat16), "replica", axis=0, tiled=True),
        lax.all_gather(stepped_mixed.astype(jnp.bfloat16), "replica", axis=1, tiled=True),
        lax.all_gather(stepped_norm.astype(jnp.bfloat16), "replica", axis=0, tiled=True),
        lax.all_gather(stepped_bias.astype(jnp.bfloat16), "replica", axis=0, tiled=True),
    )
    return (
        compute_query,
        compute_key,
        compute_value,
        compute_mixed,
        compute_norm,
        compute_bias,
        stepped_query,
        stepped_key,
        stepped_value,
        stepped_mixed,
        stepped_norm,
        stepped_bias,
        state_new_query,
        state_new_key,
        state_new_value,
        state_new_mixed,
        state_new_norm,
        state_new_bias,
    )


def exchange(n, cuts, *refs):
    vec_ref, part_refs, master_refs, memory_refs = refs[0], refs[1:5], refs[5:9], refs[9:13]
    vecs_ref, comp_refs, stepped_refs, state_refs = refs[13], refs[14:18], refs[18:22], refs[22:26]
    parts, masters, memories = refs[26:30], refs[30:34], refs[34:38]
    stage, landed, gathered = refs[38:41]
    load_sem, store_sem, vec_send, vec_recv, rs_send, rs_recv, ag_send, ag_recv = refs[41:49]

    me = lax.axis_index("replica")
    rate = n ** (-0.5)
    rows = stage.shape[2]
    span = rows * cuts
    values = [gathered if k == TURNED else comp_refs[k] for k in range(4)]
    steps = 4 * cuts

    loads = []
    for k in range(4):
        loads.append(pltpu.make_async_copy(part_refs[k], parts[k], load_sem.at[k]))
    for k in range(4):
        loads.append(pltpu.make_async_copy(memory_refs[k], memories[k], load_sem.at[4 + k]))
        loads.append(pltpu.make_async_copy(master_refs[k], masters[k], load_sem.at[8 + k]))
    for load in loads:
        load.start()
    stores = [pltpu.make_async_copy(memories[k], state_refs[k], store_sem.at[k]) for k in range(4)]
    stores += [pltpu.make_async_copy(masters[k], stepped_refs[k], store_sem.at[4 + k]) for k in range(4)]

    barrier = pltpu.get_barrier_semaphore()
    for k in range(1, n):
        pl.semaphore_signal(
            barrier, inc=1, device_id={"replica": lax.rem(me + k, n)}, device_id_type=MESH
        )

    def prepare(k):
        loads[k].wait()
        whole = parts[k][...].T if k == TURNED else parts[k][...]
        for d in range(n):
            for h in range(cuts):
                at = d * span + h * rows
                stage[k * cuts + h, d] = whole[at : at + rows, :].astype(stage.dtype)

    right = lax.rem(me + 1, n)
    left = lax.rem(me + n - 1, n)

    def sum_copy(way, t, d):
        return pltpu.make_async_remote_copy(
            src_ref=stage.at[t, d],
            dst_ref=landed.at[way, t, d],
            send_sem=rs_send.at[t, d],
            recv_sem=rs_recv.at[way, t, d],
            device_id={"replica": right if way == 0 else left},
            device_id_type=MESH,
        )

    def gather_copy(way, t, s):
        k, h = divmod(t, cuts)
        held = values[k].at[pl.ds(pl.multiple_of(s * span + h * rows, 16), rows), :]
        return pltpu.make_async_remote_copy(
            src_ref=held,
            dst_ref=held,
            send_sem=ag_send.at[way, t, s],
            recv_sem=ag_recv.at[t, s],
            device_id={"replica": right if way == 0 else left},
            device_id_type=MESH,
        )

    def raw(t):
        @pl.when(me == 0)
        def _():
            for d in range(n - 1, 0, -1):
                sum_copy(0, t, d).start()

        @pl.when(me == n - 1)
        def _():
            for d in range(n - 1):
                sum_copy(1, t, d).start()

    def relay(way, t, d):
        sum_copy(way, t, d).wait_recv()
        stage[t, d] = (
            stage[t, d].astype(jnp.float32) + landed[way, t, d].astype(jnp.float32)
        ).astype(stage.dtype)
        sum_copy(way, t, d).start()

    def relays(t):
        for k in range(n - 1):
            far = n - 1 - k
            pl.when((me > 0) & (me < far))(functools.partial(relay, 0, t, far))
            pl.when((me < n - 1) & (me > k))(functools.partial(relay, 1, t, k))

    def finish(t):
        k, h = divmod(t, cuts)
        if h == 0:
            loads[4 + 2 * k].wait()
            loads[5 + 2 * k].wait()

        def add(way):
            sum_copy(way, t, me).wait_recv()
            return landed[way, t, me].astype(jnp.float32)

        def update(*ways):
            total = stage[t, me].astype(jnp.float32)
            for way in ways:
                total = total + add(way)
            mean = total * rate
            at = slice(h * rows, (h + 1) * rows)
            state = hold_rate * memories[k][at, :] + mean
            memories[k][at, :] = state
            stepped = masters[k][at, :] - learn_rate * state
            masters[k][at, :] = stepped
            values[k][pl.ds(pl.multiple_of(me * span + h * rows, 16), rows), :] = stepped.astype(stage.dtype)

        @pl.when(me == 0)
        def _():
            update(1)
            gather_copy(0, t, me).start()

        @pl.when(me == n - 1)
        def _():
            update(0)
            gather_copy(1, t, me).start()

        @pl.when((me > 0) & (me < n - 1))
        def _():
            update(0, 1)
            gather_copy(0, t, me).start()
            gather_copy(1, t, me).start()

        if h == cuts - 1:
            stores[k].start()
            stores[4 + k].start()

    def pass_on(way, t, s):
        gather_copy(way, t, s).wait_recv()
        pl.when((me < n - 1) if way == 0 else (me > 0))(lambda: gather_copy(way, t, s).start())

    def spread(t):
        for k in range(1, n):
            pl.when(me - k >= 0)(lambda: pass_on(0, t, me - k))
            pl.when(me + k <= n - 1)(lambda: pass_on(1, t, me + k))
        k, h = divmod(t, cuts)
        if k == TURNED and h == cuts - 1:
            comp_refs[k][...] = gathered[...].astype(jnp.float32).T.astype(stage.dtype)

    def vec_copy(k):
        return pltpu.make_async_remote_copy(
            src_ref=vec_ref,
            dst_ref=vecs_ref.at[me],
            send_sem=vec_send.at[k],
            recv_sem=vec_recv.at[k],
            device_id={"replica": lax.rem(me + k, n)},
            device_id_type=MESH,
        )

    prepare(0)
    pl.semaphore_wait(barrier, n - 1)
    for h in range(min(2, steps)):
        if h % cuts == 0 and h > 0:
            prepare(h // cuts)
        raw(h)
    for k in range(1, n):
        vec_copy(k).start()
    vecs_ref[me] = vec_ref[...]
    for t in range(steps + 1):
        ahead = t + 2
        if ahead < steps:
            if ahead % cuts == 0:
                prepare(ahead // cuts)
            raw(ahead)
        if t < steps:
            relays(t)
            finish(t)
        if t >= 1:
            spread(t - 1)

    for store in stores:
        store.wait()
    for k in range(1, n):
        vec_copy(k).wait()
    for t in range(steps):
        for d in range(n):
            pl.when(me < d)(lambda: sum_copy(0, t, d).wait_send())
            pl.when(me > d)(lambda: sum_copy(1, t, d).wait_send())
            pl.when((me >= d) & (me < n - 1))(lambda: gather_copy(0, t, d).wait_send())
            pl.when((me <= d) & (me > 0))(lambda: gather_copy(1, t, d).wait_send())


def line_on_device(n, *args):
    grads, masters, memories = args[:6], args[6:12], args[12:18]
    span, inner = masters[0].shape
    cuts = 2 if span % 32 == 0 else 1
    rows = span // cuts
    wide, small = jnp.bfloat16, jnp.float32
    vec = jnp.concatenate([grads[4][0], grads[5][0], masters[4], masters[5], memories[4], memories[5]])
    vec = vec.reshape(-1, 128)
    parts = [grads[k][0] for k in ORDER]
    held = [[m[k].T if k == 3 else m[k] for k in ORDER] for m in (masters, memories)]
    room = sum(p.size * 2 for p in parts) + n * (vec.size + 8 * 128) * 4 + 2**18
    steps = 4 * cuts
    hbm = pl.BlockSpec(memory_space=pltpu.HBM)
    vmem = pl.BlockSpec(memory_space=pltpu.VMEM)
    out_shape = (
        [pltpu.VMEM((n, *vec.shape), small)]
        + [pltpu.VMEM(p.shape, wide) for p in parts]
        + [jax.ShapeDtypeStruct(m.shape, small) for m in held[0]] * 2
    )
    out = pl.pallas_call(
        functools.partial(exchange, n, cuts),
        out_shape=out_shape,
        in_specs=[vmem] + [hbm] * 12,
        out_specs=[vmem] * 5 + [hbm] * 8,
        scratch_shapes=[pltpu.VMEM(p.shape, small) for p in parts]
        + [pltpu.VMEM(m.shape, small) for m in held[0]] * 2
        + [
            pltpu.VMEM((steps, n, rows, inner), wide),
            pltpu.VMEM((2, steps, n, rows, inner), wide),
            pltpu.VMEM((n * span, inner), wide),
            pltpu.SemaphoreType.DMA((12,)),
            pltpu.SemaphoreType.DMA((8,)),
            pltpu.SemaphoreType.DMA((n,)),
            pltpu.SemaphoreType.DMA((n,)),
            pltpu.SemaphoreType.DMA((steps, n)),
            pltpu.SemaphoreType.DMA((2, steps, n)),
            pltpu.SemaphoreType.DMA((2, steps, n)),
            pltpu.SemaphoreType.DMA((steps, n)),
        ],
        compiler_params=pltpu.CompilerParams(
            collective_id=0, has_side_effects=True, vmem_limit_bytes=67_043_328 - room
        ),
    )(vec, *parts, *held[0], *held[1])
    vecs = out[0].reshape(n, -1)
    whole = grads[4].shape[1]
    place = lax.axis_index("replica") * masters[4].shape[0]
    comp, stepped, state = (
        [out[first + ORDER.index(k)] for k in range(4)] for first in (1, 5, 9)
    )
    stepped[3], state[3] = stepped[3].T, state[3].T
    for k in range(2):
        mean = jnp.sum(vecs[:, k * whole : (k + 1) * whole], axis=0) * (n ** (-0.5))
        at = 2 * whole + k * masters[4].shape[0]
        master = vecs[:, at : at + masters[4].shape[0]].reshape(-1)
        at = at + 2 * masters[4].shape[0]
        memory = vecs[:, at : at + masters[4].shape[0]].reshape(-1)
        state_all = hold_rate * memory + mean
        stepped_all = master - learn_rate * state_all
        comp.append(stepped_all.astype(wide))
        stepped.append(lax.dynamic_slice_in_dim(stepped_all, place, masters[4].shape[0]))
        state.append(lax.dynamic_slice_in_dim(state_all, place, masters[4].shape[0]))
    return (*comp, *stepped, *state)


def chosen(n, *args):
    span, inner = args[6].shape
    height, width = args[9].shape
    fits = n > 1 and span % 16 == 0 and width == span and height == inner
    fits = fits and inner % 128 == 0 and (2 * args[4].shape[1] + 4 * args[10].shape[0]) % 128 == 0
    if fits:
        return line_on_device(n, *args)
    return on_device(*args)


def solution(mesh):
    in_specs = (
        P(("unit", "replica"), None, "model"),
        P(("unit", "replica"), None, "model"),
        P(("unit", "replica"), None, "model"),
        P(("unit", "replica"), "model", None),
        P(("unit", "replica"), None),
        P(("unit", "replica"), None),
        P(("unit", "replica"), "model"),
        P(("unit", "replica"), "model"),
        P(("unit", "replica"), "model"),
        P(("unit", "model"), "replica"),
        P(("unit", "replica")),
        P(("unit", "replica")),
        P(("unit", "replica"), "model"),
        P(("unit", "replica"), "model"),
        P(("unit", "replica"), "model"),
        P(("unit", "model"), "replica"),
        P(("unit", "replica")),
        P(("unit", "replica")),
    )
    out_specs = (
        P("unit", "model"),
        P("unit", "model"),
        P("unit", "model"),
        P(("unit", "model"), None),
        P("unit"),
        P("unit"),
        P(("unit", "replica"), "model"),
        P(("unit", "replica"), "model"),
        P(("unit", "replica"), "model"),
        P(("unit", "model"), "replica"),
        P(("unit", "replica")),
        P(("unit", "replica")),
        P(("unit", "replica"), "model"),
        P(("unit", "replica"), "model"),
        P(("unit", "replica"), "model"),
        P(("unit", "model"), "replica"),
        P(("unit", "replica")),
        P(("unit", "replica")),
    )
    return jax.shard_map(
        functools.partial(chosen, mesh.shape["replica"]), mesh=mesh, in_specs=in_specs, out_specs=out_specs, check_vma=False
    )
```

```python
import functools

import jax
import jax.numpy as jnp
from jax import lax
from jax.experimental import pallas as pl
from jax.experimental.pallas import tpu as pltpu
from jax.sharding import PartitionSpec as P

MESH = pl.DeviceIdType.MESH
ORDER = (0, 3, 1, 2)
TURNED = 1

learn_rate = 0.1
hold_rate = 0.7


def on_device(
    partial_query,
    partial_key,
    partial_value,
    partial_mixed,
    partial_norm,
    partial_bias,
    master_query,
    master_key,
    master_value,
    master_mixed,
    master_norm,
    master_bias,
    memory_query,
    memory_key,
    memory_value,
    memory_mixed,
    memory_norm,
    memory_bias,
):
    mean_query, mean_key, mean_value, mean_mixed = (
        lax.psum_scatter(
            partial_query[0].astype(jnp.bfloat16), "replica", scatter_dimension=0, tiled=True
        ).astype(jnp.float32),
        lax.psum_scatter(
            partial_key[0].astype(jnp.bfloat16), "replica", scatter_dimension=0, tiled=True
        ).astype(jnp.float32),
        lax.psum_scatter(
            partial_value[0].astype(jnp.bfloat16), "replica", scatter_dimension=0, tiled=True
        ).astype(jnp.float32),
        lax.psum_scatter(
            partial_mixed[0].astype(jnp.bfloat16), "replica", scatter_dimension=1, tiled=True
        ).astype(jnp.float32),
    )
    whole_norm, whole_bias = lax.psum((partial_norm[0], partial_bias[0]), "replica")
    place = lax.axis_index("replica")
    mean_norm = lax.dynamic_slice_in_dim(
        whole_norm, place * master_norm.shape[0], master_norm.shape[0]
    )
    mean_bias = lax.dynamic_slice_in_dim(
        whole_bias, place * master_bias.shape[0], master_bias.shape[0]
    )
    mean_rate = lax.axis_size("replica") ** (-0.5)
    mean_query = mean_query * mean_rate
    mean_key = mean_key * mean_rate
    mean_value = mean_value * mean_rate
    mean_mixed = mean_mixed * mean_rate
    mean_norm = mean_norm * mean_rate
    mean_bias = mean_bias * mean_rate
    state_new_query = hold_rate * memory_query + mean_query
    stepped_query = master_query - learn_rate * state_new_query
    state_new_key = hold_rate * memory_key + mean_key
    stepped_key = master_key - learn_rate * state_new_key
    state_new_value = hold_rate * memory_value + mean_value
    stepped_value = master_value - learn_rate * state_new_value
    state_new_mixed = hold_rate * memory_mixed + mean_mixed
    stepped_mixed = master_mixed - learn_rate * state_new_mixed
    state_new_norm = hold_rate * memory_norm + mean_norm
    stepped_norm = master_norm - learn_rate * state_new_norm
    state_new_bias = hold_rate * memory_bias + mean_bias
    stepped_bias = master_bias - learn_rate * state_new_bias
    compute_query, compute_key, compute_value, compute_mixed, compute_norm, compute_bias = (
        lax.all_gather(stepped_query.astype(jnp.bfloat16), "replica", axis=0, tiled=True),
        lax.all_gather(stepped_key.astype(jnp.bfloat16), "replica", axis=0, tiled=True),
        lax.all_gather(stepped_value.astype(jnp.bfloat16), "replica", axis=0, tiled=True),
        lax.all_gather(stepped_mixed.astype(jnp.bfloat16), "replica", axis=1, tiled=True),
        lax.all_gather(stepped_norm.astype(jnp.bfloat16), "replica", axis=0, tiled=True),
        lax.all_gather(stepped_bias.astype(jnp.bfloat16), "replica", axis=0, tiled=True),
    )
    return (
        compute_query,
        compute_key,
        compute_value,
        compute_mixed,
        compute_norm,
        compute_bias,
        stepped_query,
        stepped_key,
        stepped_value,
        stepped_mixed,
        stepped_norm,
        stepped_bias,
        state_new_query,
        state_new_key,
        state_new_value,
        state_new_mixed,
        state_new_norm,
        state_new_bias,
    )


def exchange(n, cuts, *refs):
    vec_ref, part_refs, master_refs, memory_refs = refs[0], refs[1:5], refs[5:9], refs[9:13]
    vecs_ref, comp_refs, stepped_refs, state_refs = refs[13], refs[14:18], refs[18:22], refs[22:26]
    parts, masters, memories = refs[26:30], refs[30:34], refs[34:38]
    stage, landed, gathered = refs[38:41]
    load_sem, store_sem, vec_send, vec_recv, rs_send, rs_recv, ag_send, ag_recv = refs[41:49]

    me = lax.axis_index("replica")
    rate = n ** (-0.5)
    rows = stage.shape[2]
    span = rows * cuts
    values = [gathered if k == TURNED else comp_refs[k] for k in range(4)]
    steps = 4 * cuts

    loads = []
    for k in range(4):
        loads.append(pltpu.make_async_copy(part_refs[k], parts[k], load_sem.at[k]))
    for k in range(4):
        loads.append(pltpu.make_async_copy(memory_refs[k], memories[k], load_sem.at[4 + k]))
        loads.append(pltpu.make_async_copy(master_refs[k], masters[k], load_sem.at[8 + k]))
    for load in loads:
        load.start()
    stores = [pltpu.make_async_copy(memories[k], state_refs[k], store_sem.at[k]) for k in range(4)]
    stores += [pltpu.make_async_copy(masters[k], stepped_refs[k], store_sem.at[4 + k]) for k in range(4)]

    barrier = pltpu.get_barrier_semaphore()
    for k in range(1, n):
        pl.semaphore_signal(
            barrier, inc=1, device_id={"replica": lax.rem(me + k, n)}, device_id_type=MESH
        )

    def prepare(k):
        loads[k].wait()
        whole = parts[k][...].T if k == TURNED else parts[k][...]
        for d in range(n):
            for h in range(cuts):
                at = d * span + h * rows
                stage[k * cuts + h, d] = whole[at : at + rows, :].astype(stage.dtype)

    right = lax.rem(me + 1, n)
    left = lax.rem(me + n - 1, n)

    def sum_copy(way, t, d):
        return pltpu.make_async_remote_copy(
            src_ref=stage.at[t, d],
            dst_ref=landed.at[way, t, d],
            send_sem=rs_send.at[t, d],
            recv_sem=rs_recv.at[way, t, d],
            device_id={"replica": right if way == 0 else left},
            device_id_type=MESH,
        )

    def gather_copy(way, t, s):
        k, h = divmod(t, cuts)
        held = values[k].at[pl.ds(pl.multiple_of(s * span + h * rows, 16), rows), :]
        return pltpu.make_async_remote_copy(
            src_ref=held,
            dst_ref=held,
            send_sem=ag_send.at[way, t, s],
            recv_sem=ag_recv.at[t, s],
            device_id={"replica": right if way == 0 else left},
            device_id_type=MESH,
        )

    def raw(t):
        @pl.when(me == 0)
        def _():
            for d in range(n - 1, 0, -1):
                sum_copy(0, t, d).start()

        @pl.when(me == n - 1)
        def _():
            for d in range(n - 1):
                sum_copy(1, t, d).start()

    def relay(way, t, d):
        sum_copy(way, t, d).wait_recv()
        stage[t, d] = (
            stage[t, d].astype(jnp.float32) + landed[way, t, d].astype(jnp.float32)
        ).astype(stage.dtype)
        sum_copy(way, t, d).start()

    def relays(t):
        for k in range(n - 1):
            far = n - 1 - k
            pl.when((me > 0) & (me < far))(functools.partial(relay, 0, t, far))
            pl.when((me < n - 1) & (me > k))(functools.partial(relay, 1, t, k))

    def finish(t):
        k, h = divmod(t, cuts)
        if h == 0:
            loads[4 + 2 * k].wait()
            loads[5 + 2 * k].wait()

        def add(way):
            sum_copy(way, t, me).wait_recv()
            return landed[way, t, me].astype(jnp.float32)

        def update(*ways):
            total = stage[t, me].astype(jnp.float32)
            for way in ways:
                total = total + add(way)
            mean = total * rate
            at = slice(h * rows, (h + 1) * rows)
            state = hold_rate * memories[k][at, :] + mean
            memories[k][at, :] = state
            stepped = masters[k][at, :] - learn_rate * state
            masters[k][at, :] = stepped
            values[k][pl.ds(pl.multiple_of(me * span + h * rows, 16), rows), :] = stepped.astype(stage.dtype)

        @pl.when(me == 0)
        def _():
            update(1)
            gather_copy(0, t, me).start()

        @pl.when(me == n - 1)
        def _():
            update(0)
            gather_copy(1, t, me).start()

        @pl.when((me > 0) & (me < n - 1))
        def _():
            update(0, 1)
            gather_copy(0, t, me).start()
            gather_copy(1, t, me).start()

        if h == cuts - 1:
            stores[k].start()
            stores[4 + k].start()

    def pass_on(way, t, s):
        gather_copy(way, t, s).wait_recv()
        pl.when((me < n - 1) if way == 0 else (me > 0))(lambda: gather_copy(way, t, s).start())

    def spread(t):
        for k in range(1, n):
            pl.when(me - k >= 0)(lambda: pass_on(0, t, me - k))
            pl.when(me + k <= n - 1)(lambda: pass_on(1, t, me + k))
        k, h = divmod(t, cuts)
        if k == TURNED and h == cuts - 1:
            comp_refs[k][...] = gathered[...].astype(jnp.float32).T.astype(stage.dtype)

    def vec_copy(k):
        return pltpu.make_async_remote_copy(
            src_ref=vec_ref,
            dst_ref=vecs_ref.at[me],
            send_sem=vec_send.at[k],
            recv_sem=vec_recv.at[k],
            device_id={"replica": lax.rem(me + k, n)},
            device_id_type=MESH,
        )

    prepare(0)
    pl.semaphore_wait(barrier, n - 1)
    for h in range(min(2, steps)):
        if h % cuts == 0 and h > 0:
            prepare(h // cuts)
        raw(h)
    for k in range(1, n):
        vec_copy(k).start()
    vecs_ref[me] = vec_ref[...]
    for t in range(steps + 1):
        ahead = t + 2
        if ahead < steps:
            if ahead % cuts == 0:
                prepare(ahead // cuts)
            raw(ahead)
        if t < steps:
            relays(t)
            finish(t)
        if t >= 1:
            spread(t - 1)

    for store in stores:
        store.wait()
    for k in range(1, n):
        vec_copy(k).wait()
    for t in range(steps):
        for d in range(n):
            pl.when(me < d)(lambda: sum_copy(0, t, d).wait_send())
            pl.when(me > d)(lambda: sum_copy(1, t, d).wait_send())
            pl.when((me >= d) & (me < n - 1))(lambda: gather_copy(0, t, d).wait_send())
            pl.when((me <= d) & (me > 0))(lambda: gather_copy(1, t, d).wait_send())


def line_on_device(n, *args):
    grads, masters, memories = args[:6], args[6:12], args[12:18]
    span, inner = masters[0].shape
    cuts = 1
    rows = span // cuts
    wide, small = jnp.bfloat16, jnp.float32
    vec = jnp.concatenate([grads[4][0], grads[5][0], masters[4], masters[5], memories[4], memories[5]])
    vec = vec.reshape(-1, 128)
    parts = [grads[k][0] for k in ORDER]
    held = [[m[k].T if k == 3 else m[k] for k in ORDER] for m in (masters, memories)]
    room = sum(p.size * 2 for p in parts) + n * (vec.size + 8 * 128) * 4 + 2**18
    steps = 4 * cuts
    hbm = pl.BlockSpec(memory_space=pltpu.HBM)
    vmem = pl.BlockSpec(memory_space=pltpu.VMEM)
    out_shape = (
        [pltpu.VMEM((n, *vec.shape), small)]
        + [pltpu.VMEM(p.shape, wide) for p in parts]
        + [jax.ShapeDtypeStruct(m.shape, small) for m in held[0]] * 2
    )
    out = pl.pallas_call(
        functools.partial(exchange, n, cuts),
        out_shape=out_shape,
        in_specs=[vmem] + [hbm] * 12,
        out_specs=[vmem] * 5 + [hbm] * 8,
        scratch_shapes=[pltpu.VMEM(p.shape, small) for p in parts]
        + [pltpu.VMEM(m.shape, small) for m in held[0]] * 2
        + [
            pltpu.VMEM((steps, n, rows, inner), wide),
            pltpu.VMEM((2, steps, n, rows, inner), wide),
            pltpu.VMEM((n * span, inner), wide),
            pltpu.SemaphoreType.DMA((12,)),
            pltpu.SemaphoreType.DMA((8,)),
            pltpu.SemaphoreType.DMA((n,)),
            pltpu.SemaphoreType.DMA((n,)),
            pltpu.SemaphoreType.DMA((steps, n)),
            pltpu.SemaphoreType.DMA((2, steps, n)),
            pltpu.SemaphoreType.DMA((2, steps, n)),
            pltpu.SemaphoreType.DMA((steps, n)),
        ],
        compiler_params=pltpu.CompilerParams(
            collective_id=0, has_side_effects=True, vmem_limit_bytes=67_043_328 - room
        ),
    )(vec, *parts, *held[0], *held[1])
    vecs = out[0].reshape(n, -1)
    whole = grads[4].shape[1]
    place = lax.axis_index("replica") * masters[4].shape[0]
    comp, stepped, state = (
        [out[first + ORDER.index(k)] for k in range(4)] for first in (1, 5, 9)
    )
    stepped[3], state[3] = stepped[3].T, state[3].T
    for k in range(2):
        mean = jnp.sum(vecs[:, k * whole : (k + 1) * whole], axis=0) * (n ** (-0.5))
        at = 2 * whole + k * masters[4].shape[0]
        master = vecs[:, at : at + masters[4].shape[0]].reshape(-1)
        at = at + 2 * masters[4].shape[0]
        memory = vecs[:, at : at + masters[4].shape[0]].reshape(-1)
        state_all = hold_rate * memory + mean
        stepped_all = master - learn_rate * state_all
        comp.append(stepped_all.astype(wide))
        stepped.append(lax.dynamic_slice_in_dim(stepped_all, place, masters[4].shape[0]))
        state.append(lax.dynamic_slice_in_dim(state_all, place, masters[4].shape[0]))
    return (*comp, *stepped, *state)


def chosen(n, *args):
    span, inner = args[6].shape
    height, width = args[9].shape
    fits = n > 1 and span % 16 == 0 and width == span and height == inner
    fits = fits and inner % 128 == 0 and (2 * args[4].shape[1] + 4 * args[10].shape[0]) % 128 == 0
    if fits:
        return line_on_device(n, *args)
    return on_device(*args)


def solution(mesh):
    in_specs = (
        P(("unit", "replica"), None, "model"),
        P(("unit", "replica"), None, "model"),
        P(("unit", "replica"), None, "model"),
        P(("unit", "replica"), "model", None),
        P(("unit", "replica"), None),
        P(("unit", "replica"), None),
        P(("unit", "replica"), "model"),
        P(("unit", "replica"), "model"),
        P(("unit", "replica"), "model"),
        P(("unit", "model"), "replica"),
        P(("unit", "replica")),
        P(("unit", "replica")),
        P(("unit", "replica"), "model"),
        P(("unit", "replica"), "model"),
        P(("unit", "replica"), "model"),
        P(("unit", "model"), "replica"),
        P(("unit", "replica")),
        P(("unit", "replica")),
    )
    out_specs = (
        P("unit", "model"),
        P("unit", "model"),
        P("unit", "model"),
        P(("unit", "model"), None),
        P("unit"),
        P("unit"),
        P(("unit", "replica"), "model"),
        P(("unit", "replica"), "model"),
        P(("unit", "replica"), "model"),
        P(("unit", "model"), "replica"),
        P(("unit", "replica")),
        P(("unit", "replica")),
        P(("unit", "replica"), "model"),
        P(("unit", "replica"), "model"),
        P(("unit", "replica"), "model"),
        P(("unit", "model"), "replica"),
        P(("unit", "replica")),
        P(("unit", "replica")),
    )
    return jax.shard_map(
        functools.partial(chosen, mesh.shape["replica"]), mesh=mesh, in_specs=in_specs, out_specs=out_specs, check_vma=False
    )
```
